256 devices in a mesh: clips: 2 (over z), tile: 16 (over y, core), tm: 8 (over x).
Axes of the slice: x: 8, y: 8, z: 2, core: 2. Of those that a mesh axis runs over, the one named last changes fastest.
The devices are a block of a 8x8x16 slice.
Arguments:
- clip_frames: bfloat16 [32, 64, 128, 256], P(('clips', 'tm'), 'tile'), parts along dimension 0, may hold values from -6 to 6
- weight_first: bfloat16 [3, 3, 3, 256, 256], replicated, may hold values from -0.078125 to 0.078125
- bias_first: float32 [256], replicated, may hold values from -3 to 3
- weight_second: bfloat16 [3, 3, 3, 256, 256], replicated, may hold values from -0.078125 to 0.078125
- bias_second: float32 [256], replicated, may hold values from -3 to 3
Outputs:
- pooled_frames: bfloat16 [16, 64, 128, 256], P(('clips', 'tm'), 'tile'), parts along dimension 0
The draws below stay inside these ranges and needn't reach their ends.
There are 2 independent parts, one for each index of `clips`. The reference program is written for one: setup_inputs(seed, part) draws one part's arguments, and reference() takes and returns one part's arrays. A program takes and returns all parts, laid end to end along the dimension named above; an argument that names none is the same for every part. Nothing has to cross between parts.
All inputs are finite; a program needn't handle non-finite values.
Results may differ from the reference program's by a relative error of at most 0.0029.
Values may be sent and summed in bfloat16 or wider, within the bound.
A program may use at most 128 MiB of HBM per device.

```python
import jax
import jax.numpy as jnp

C = 256
W = 128
NT = 16
H = 64


def shard_levels(key, dims, cuts, smallest, top_value):
    def one(position, shards_of):
        steps = jax.random.uniform(jax.random.fold_in(jax.random.fold_in(key, 6), position), (shards_of,), jnp.float32, smallest / len(cuts), top_value / len(cuts))
        return jnp.repeat(jnp.exp(steps), dims[position] // shards_of).reshape((-1,) + (1,) * (len(dims) - position - 1))

    gain = one(*cuts[0])
    for cut in cuts[1:]:
        gain = gain * one(*cut)
    return gain


def gaussian(key, shape, width, limit, split=(), held_as=jnp.bfloat16):
    entries = jax.random.normal(key, shape, jnp.float32) * width
    if len(split) > 0:
        entries = shard_levels(key, shape, split, -0.22, 0.18) * entries
    return jnp.clip(entries, min=-limit, max=limit).astype(held_as)


def setup_inputs(seed: int = 0, part: int = 0) -> dict:
    splits = jax.random.split(jax.random.key(seed), 6)
    own_keys = jax.random.split(jax.random.fold_in(splits[5], part), 6)
    return {
        "clip_frames": gaussian(own_keys[0], (NT, H, W, C), 1.0, 6.0, ((0, 8), (1, 16))),
        "weight_first": gaussian(splits[1], (3, 3, 3, C, C), (27 * C) ** -0.5, 0.078125),
        "bias_first": gaussian(splits[2], (C,), 0.5, 3.0, (), jnp.float32),
        "weight_second": gaussian(splits[3], (3, 3, 3, C, C), (27 * C) ** -0.5, 0.078125),
        "bias_second": gaussian(splits[4], (C,), 0.5, 3.0, (), jnp.float32),
    }


def causal_taps(padded_input, weight, bias):
    frame_count = padded_input.shape[0] - 2
    row_count = padded_input.shape[1] - 2
    width_cells = padded_input.shape[2]
    channels = padded_input.shape[3]
    widened = jnp.pad(padded_input, ((0, 0), (0, 0), (1, 1), (0, 0)))
    accumulated = jnp.zeros((frame_count, row_count, width_cells, channels), jnp.float32) + bias
    for depth_tap in range(3):
        for row_tap in range(3):
            slab_taps = jnp.concatenate([widened[depth_tap:depth_tap + frame_count, row_tap:row_tap + row_count, width_tap:width_tap + width_cells] for width_tap in range(3)], axis=-1)
            product = jnp.dot(slab_taps.reshape(-1, 3 * channels), weight[depth_tap, row_tap].reshape(3 * channels, channels), preferred_element_type=jnp.float32)
            accumulated = accumulated + product.reshape(frame_count, row_count, width_cells, channels)
    return accumulated


def reference(clip_frames, weight_first, bias_first, weight_second, bias_second):
    padded_input = jnp.pad(clip_frames, ((2, 0), (1, 1), (0, 0), (0, 0)))
    hidden = jax.nn.silu(causal_taps(padded_input, weight_first, bias_first)).astype(jnp.bfloat16)
    padded_hidden = jnp.pad(hidden, ((2, 0), (1, 1), (0, 0), (0, 0)))
    summed = clip_frames.astype(jnp.float32) + causal_taps(padded_hidden, weight_second, bias_second)
    return ((summed[0::2] + summed[1::2]) * 0.5).astype(jnp.bfloat16)
```

```python
import jax
import jax.numpy as jnp
from jax import lax
from jax.experimental import pallas as pl
from jax.experimental.pallas import tpu as pltpu
from jax.sharding import PartitionSpec as P

MESH = pl.DeviceIdType.MESH
PAD = 8
F32 = jnp.float32
BF16 = jnp.bfloat16


def mm(a, b):
    return jnp.dot(a, b, preferred_element_type=F32)


def bounds(width):
    step = width // 4
    xs = [0, step + 16, 2 * step + 16, 3 * step + 16, width]
    hs = [0, step, 2 * step, 3 * step, width]
    os = [0, step - 16, 2 * step - 16, 3 * step - 16, width]
    return xs, hs, os


def kernel(
    x_hbm, w1_hbm, b1_ref, w2_hbm, b2_ref, out_hbm,
    xo, xh, w1, w2, w01, acc, hs, oq, nq, ob, ns, nr, outv,
    ld, st, xs_s, xs_r, ro_s, ro_r, fw_s, fw_r, he_s, he_r, n_s, n_r,
):
    frames, rows, width, chans = x_hbm.shape
    xb, hb, pb = bounds(width)
    chunks = len(xb) - 1
    i, j = lax.axis_index("tm"), lax.axis_index("tile")
    ni, nj = lax.axis_size("tm"), lax.axis_size("tile")
    has_prev, has_next = i > 0, i < ni - 1
    has_up, has_dn = j > 0, j < nj - 1
    prev, nxt = {"tm": i - 1}, {"tm": i + 1}
    up, dn = {"tile": j - 1}, {"tile": j + 1}
    last = rows

    def local(src, dst, sem):
        return pltpu.make_async_copy(src, dst, sem)

    def remote(src, dst, ssem, rsem, dev):
        return pltpu.make_async_remote_copy(
            src_ref=src, dst_ref=dst, send_sem=ssem, recv_sem=rsem, device_id=dev, device_id_type=MESH
        )

    load_x = local(x_hbm, xo.at[:, 1 : rows + 1], ld.at[0])
    load_w1 = local(w1_hbm, w1, ld.at[1])
    load_w2 = local(w2_hbm, w2, ld.at[2])
    load_x.start()
    load_w1.start()
    load_w2.start()

    barrier = pltpu.get_barrier_semaphore()
    for cond, dev in ((has_prev, prev), (has_up, up), (has_dn, dn)):
        @pl.when(cond)
        def _(dev=dev):
            pl.semaphore_signal(barrier, inc=1, device_id=dev, device_id_type=MESH)

    for buf in (oq, nq):
        for q, at in ((0, 0), (2, PAD + width)):
            buf[q, :, at : at + PAD, :] = jnp.zeros((rows, PAD, chans), F32)
    for q, at in ((0, 0), (2, PAD + width)):
        acc[q, :, :, at : at + PAD, :] = jnp.zeros((frames, rows, PAD, chans), F32)

    @pl.when(jnp.logical_not(has_prev))
    def _():
        xh[...] = jnp.zeros(xh.shape, BF16)
        nr[...] = jnp.zeros(nr.shape, BF16)

    for cond, row in ((has_up, 0), (has_dn, last + 1)):
        @pl.when(jnp.logical_not(cond))
        def _(row=row):
            zero = jnp.zeros((frames, width, chans), BF16)
            xo[:, row] = zero
            xh[:, row] = zero
            hs[:, row] = zero

    load_x.wait()
    pl.semaphore_wait(barrier, sum(cond.astype(jnp.int32) for cond in (has_next, has_up, has_dn)))

    def rowcopy(buf, c0, c1, s, r, k, down):
        if down:
            return remote(buf.at[:, last, c0:c1], buf.at[:, 0, c0:c1], s.at[k], r.at[k], dn)
        return remote(buf.at[:, 1, c0:c1], buf.at[:, last + 1, c0:c1], s.at[k], r.at[k], up)

    own_up = rowcopy(xo, 0, width, ro_s, ro_r, 0, False)
    own_dn = rowcopy(xo, 0, width, ro_s, ro_r, 1, True)
    edges, middle = [], []
    for c in range(chunks):
        c0, c1 = xb[c], xb[c + 1]
        edges.append([
            remote(xo.at[:, row, c0:c1], xh.at[:, row, c0:c1], xs_s.at[3 * c + k], xs_r.at[3 * c + k], nxt)
            for k, row in enumerate((1, last))
        ])
        middle.append(
            remote(xo.at[:, 2:last, c0:c1], xh.at[:, 2:last, c0:c1], xs_s.at[3 * c + 2], xs_r.at[3 * c + 2], nxt)
        )
    fwd = [
        (rowcopy(xh, xb[c], xb[c + 1], fw_s, fw_r, 2 * c, False),
         rowcopy(xh, xb[c], xb[c + 1], fw_s, fw_r, 2 * c + 1, True))
        for c in range(chunks)
    ]
    hid = [
        (rowcopy(hs, hb[c], hb[c + 1], he_s, he_r, 2 * c, False),
         rowcopy(hs, hb[c], hb[c + 1], he_s, he_r, 2 * c + 1, True))
        for c in range(chunks)
    ]
    part = [
        remote(ns.at[:, pb[c] : pb[c + 1]], nr.at[:, pb[c] : pb[c + 1]], n_s.at[c], n_r.at[c], nxt)
        for c in range(chunks)
    ]

    @pl.when(has_next)
    def _():
        for pair in edges:
            for copy in pair:
                copy.start()
        for copy in middle:
            copy.start()

    @pl.when(has_up)
    def _():
        own_up.start()

    @pl.when(has_dn)
    def _():
        own_dn.start()

    load_w2.wait()
    w01[...] = (w2[0].astype(F32) + w2[1].astype(F32)).astype(BF16)
    load_w1.wait()

    @pl.when(has_dn)
    def _():
        own_up.wait_recv()

    @pl.when(has_up)
    def _():
        own_dn.wait_recv()

    def forward(c):
        @pl.when(has_prev)
        def _():
            for copy in edges[c]:
                copy.wait_recv()

        @pl.when(has_prev & has_up)
        def _():
            fwd[c][0].start()

        @pl.when(has_prev & has_dn)
        def _():
            fwd[c][1].start()

    def own_tap(q):
        both = first = None
        for p in range(3):
            v = xo[:, p : p + rows].reshape(frames * rows * width, chans)
            a = mm(v, w1[2, p, q])
            b = mm(v[: rows * width], w1[1, p, q])
            both = a if both is None else both + a
            first = b if first is None else first + b
        inside = slice(PAD, PAD + width)
        acc[q, 0, :, inside, :] = both[: rows * width].reshape(rows, width, chans)
        acc[q, 1, :, inside, :] = (both[rows * width :] + first).reshape(rows, width, chans)

    for c in range(chunks):
        forward(c)
        if c < 3:
            own_tap(c)

    def shifted_sum(ref, c0, c1):
        return sum(ref[q, ..., PAD - 1 + q + c0 : PAD - 1 + q + c1, :] for q in range(3))

    bias1 = b1_ref[...].reshape(1, 1, chans)
    bias2 = b2_ref[...].reshape(1, 1, chans)

    def first_conv(c):
        @pl.when(has_prev)
        def _():
            middle[c].wait_recv()

        @pl.when(has_prev & has_dn)
        def _():
            fwd[c][0].wait_recv()

        @pl.when(has_prev & has_up)
        def _():
            fwd[c][1].wait_recv()

        c0, c1 = xb[c], xb[c + 1]
        size = rows * (c1 - c0)
        for q in range(3):
            both = second = None
            for p in range(3):
                v = xh[:, p : p + rows, c0:c1].reshape(frames * size, chans)
                a = mm(v, w1[0, p, q])
                b = mm(v[size:], w1[1, p, q])
                both = a if both is None else both + a
                second = b if second is None else second + b
            inside = slice(PAD + c0, PAD + c1)
            acc[q, 0, :, inside, :] += (both[:size] + second).reshape(rows, c1 - c0, chans)
            acc[q, 1, :, inside, :] += both[size:].reshape(rows, c1 - c0, chans)
        h0, h1 = hb[c], hb[c + 1]
        y = [shifted_sum(acc.at[:, f], h0, h1) + bias1 for f in range(2)]
        y = [(v / (1.0 + jnp.exp(-v))).astype(BF16) for v in y]
        hs[0, 1 : rows + 1, h0:h1] = y[0]
        hs[1, 1 : rows + 1, h0:h1] = (y[0].astype(F32) + y[1].astype(F32)).astype(BF16)

        @pl.when(has_up)
        def _():
            hid[c][0].start()

        @pl.when(has_dn)
        def _():
            hid[c][1].start()

    def second_conv(c):
        @pl.when(has_dn)
        def _():
            hid[c][0].wait_recv()

        @pl.when(has_up)
        def _():
            hid[c][1].wait_recv()

        h0, h1 = hb[c], hb[c + 1]
        size = rows * (h1 - h0)
        for q in range(3):
            one = two = mix = None
            for p in range(3):
                v = hs[0, p : p + rows, h0:h1].reshape(size, chans)
                u = hs[1, p : p + rows, h0:h1].reshape(size, chans)
                a, b, d = mm(v, w2[1, p, q]), mm(u, w2[2, p, q]), mm(u, w01[p, q])
                one = a if one is None else one + a
                two = b if two is None else two + b
                mix = d if mix is None else mix + d
            inside = slice(PAD + h0, PAD + h1)
            oq[q, :, inside, :] = (one + two).reshape(rows, h1 - h0, chans)
            nq[q, :, inside, :] = (mix - one).reshape(rows, h1 - h0, chans)
        p0, p1 = pb[c], pb[c + 1]
        ns[:, p0:p1] = shifted_sum(nq, p0, p1).astype(BF16)

        @pl.when(has_next)
        def _():
            part[c].start()

        own = xo[0, 1 : rows + 1, p0:p1].astype(F32) + xo[1, 1 : rows + 1, p0:p1].astype(F32)
        ob[:, p0:p1] = 0.5 * (shifted_sum(oq, p0, p1) + own) + bias2

    first_conv(0)
    for c in range(1, chunks):
        first_conv(c)
        second_conv(c - 1)
    second_conv(chunks - 1)

    stores = []
    for c in range(chunks):
        @pl.when(has_prev)
        def _():
            part[c].wait_recv()

        p0, p1 = pb[c], pb[c + 1]
        outv[:, p0:p1] = (ob[:, p0:p1] + 0.5 * nr[:, p0:p1].astype(F32)).astype(BF16)
        store = local(outv.at[:, p0:p1], out_hbm.at[0, :, p0:p1], st.at[c])
        store.start()
        stores.append(store)

    @pl.when(has_next)
    def _():
        for c in range(chunks):
            for copy in (*edges[c], middle[c], part[c]):
                copy.wait_send()

    @pl.when(has_up)
    def _():
        own_up.wait_send()
        for c in range(chunks):
            hid[c][0].wait_send()

    @pl.when(has_dn)
    def _():
        own_dn.wait_send()
        for c in range(chunks):
            hid[c][1].wait_send()

    @pl.when(has_prev & has_up)
    def _():
        for c in range(chunks):
            fwd[c][0].wait_send()

    @pl.when(has_prev & has_dn)
    def _():
        for c in range(chunks):
            fwd[c][1].wait_send()

    for store in stores:
        store.wait()


def shards(x, w1, b1, w2, b2):
    frames, rows, width, chans = x.shape
    chunks = len(bounds(width)[0]) - 1
    dma = pltpu.SemaphoreType.DMA
    hbm, vmem = pl.BlockSpec(memory_space=pltpu.HBM), pl.BlockSpec(memory_space=pltpu.VMEM)
    extended = pltpu.VMEM((frames, rows + 2, width, chans), BF16)
    taps = pltpu.VMEM((3, rows, width + 2 * PAD, chans), F32)
    flat = pltpu.VMEM((rows, width, chans), BF16)
    return pl.pallas_call(
        kernel,
        out_shape=jax.ShapeDtypeStruct((1, rows, width, chans), BF16),
        in_specs=[hbm, hbm, vmem, hbm, vmem],
        out_specs=hbm,
        scratch_shapes=[
            extended, extended,
            pltpu.VMEM(w1.shape, BF16), pltpu.VMEM(w2.shape, BF16), pltpu.VMEM(w2.shape[1:], BF16),
            pltpu.VMEM((3, frames, rows, width + 2 * PAD, chans), F32),
            extended, taps, taps, pltpu.VMEM((rows, width, chans), F32),
            flat, flat, flat,
            dma((3,)), dma((chunks,)),
            dma((3 * chunks,)), dma((3 * chunks,)),
            dma((2,)), dma((2,)),
            dma((2 * chunks,)), dma((2 * chunks,)),
            dma((2 * chunks,)), dma((2 * chunks,)),
            dma((chunks,)), dma((chunks,)),
        ],
        compiler_params=pltpu.CompilerParams(
            collective_id=0, has_side_effects=True, vmem_limit_bytes=67043328
        ),
    )(x, w1, b1.reshape(1, chans), w2, b2.reshape(1, chans))


def solution(mesh):
    spec = P(("clips", "tm"), "tile", None, None)
    return jax.shard_map(shards, mesh=mesh, in_specs=(spec, P(), P(), P(), P()), out_specs=spec, check_vma=False)
```

```python
import functools

import jax
import jax.numpy as jnp
from jax import lax
from jax.experimental import pallas as pl
from jax.experimental.pallas import tpu as pltpu
from jax.sharding import PartitionSpec as P

MESH = pl.DeviceIdType.MESH
PAD = 8
F32 = jnp.float32
BF16 = jnp.bfloat16


def matmuls(jobs):
    units = range(len(jobs))
    for m in units:
        pltpu.matmul_push_rhs(jobs[m][0][0](), staging_register=0, mxu_index=m)
    for k in range(max(len(job) for job in jobs)):
        for m in units:
            if k + 1 < len(jobs[m]):
                pltpu.matmul_push_rhs(jobs[m][k + 1][0](), staging_register=(k + 1) % 2, mxu_index=m)
        for m in units:
            if k < len(jobs[m]):
                for n, (acc, left) in enumerate(jobs[m][k][1]):
                    pltpu.matmul_acc_lhs(acc, left(), load_staged_rhs=k % 2 if n == 0 else None)


def accumulators(body, size, count):
    spec = [pltpu.ACC(m)((size, 256), F32) for m in (0, 1) for _ in range(count)]
    pl.run_scoped(lambda *accs: body(accs[:count], accs[count:]), *spec)


def bounds(width):
    step = width // 4
    xs = [0, step + 16, 2 * step + 16, 3 * step + 16, width]
    hs = [0, step, 2 * step, 3 * step, width]
    os = [0, step - 16, 2 * step - 16, 3 * step - 16, width]
    return xs, hs, os


def kernel(
    x_hbm, w1_hbm, b1_ref, w2_hbm, b2_ref, out,
    xo, xh, w1, w2, w01, acc, hs, oq, nq, ob, ns, nr,
    ld, ready, xs_s, xs_r, ro_s, ro_r, fw_s, fw_r, he_s, he_r, n_s, n_r,
):
    frames, rows, width, chans = x_hbm.shape
    xb, hb, pb = bounds(width)
    chunks = len(xb) - 1
    i, j = lax.axis_index("tm"), lax.axis_index("tile")
    ni, nj = lax.axis_size("tm"), lax.axis_size("tile")
    has_prev, has_next = i > 0, i < ni - 1
    has_up, has_dn = j > 0, j < nj - 1
    prev, nxt = {"tm": i - 1}, {"tm": i + 1}
    up, dn = {"tile": j - 1}, {"tile": j + 1}
    last = rows

    def local(src, dst, sem):
        return pltpu.make_async_copy(src, dst, sem)

    def remote(src, dst, ssem, rsem, dev):
        return pltpu.make_async_remote_copy(
            src_ref=src, dst_ref=dst, send_sem=ssem, recv_sem=rsem, device_id=dev, device_id_type=MESH
        )

    load_x = local(x_hbm, xo.at[:, 1 : rows + 1], ld.at[0])
    load_w1_own = local(w1_hbm.at[1:3], w1.at[1:3], ld.at[1])
    load_w1_prev = local(w1_hbm.at[0], w1.at[0], ld.at[2])
    load_w2 = local(w2_hbm, w2, ld.at[3])
    load_x.start()
    load_w1_own.start()
    load_w1_prev.start()
    load_w2.start()

    barrier = pltpu.get_barrier_semaphore()
    odd = lax.rem(j, 2) == 1
    even = jnp.logical_not(odd)
    for cond, dev in ((has_prev, prev), (has_up & odd, up), (has_dn & odd, dn)):
        @pl.when(cond)
        def _(dev=dev):
            pl.semaphore_signal(barrier, inc=1, device_id=dev, device_id_type=MESH)

    for buf in (oq, nq):
        for q, at in ((0, 0), (2, PAD + width)):
            buf[q, :, at : at + PAD, :] = jnp.zeros((rows, PAD, chans), F32)
    for q, at in ((0, 0), (2, PAD + width)):
        acc[q, :, :, at : at + PAD, :] = jnp.zeros((frames, rows, PAD, chans), F32)

    @pl.when(jnp.logical_not(has_prev))
    def _():
        nr[...] = jnp.zeros(nr.shape, BF16)

    for cond, row in ((has_up, 0), (has_dn, last + 1)):
        @pl.when(jnp.logical_not(cond))
        def _(row=row):
            zero = jnp.zeros((frames, width, chans), BF16)
            xo[:, row] = zero
            xh[:, row] = zero
            hs[:, row] = zero

    accumulators(lambda unit0, unit1: [pltpu.matmul_pop(a) for a in (*unit0, *unit1)] and None, 1024, 1)
    load_x.wait()
    peers = sum(cond.astype(jnp.int32) for cond in (has_next, has_up & even, has_dn & even))

    @pl.when(peers > 0)
    def _():
        pl.semaphore_wait(barrier, peers)

    def rowcopy(buf, c0, c1, s, r, k, down):
        if down:
            return remote(buf.at[:, last, c0:c1], buf.at[:, 0, c0:c1], s.at[k], r.at[k], dn)
        return remote(buf.at[:, 1, c0:c1], buf.at[:, last + 1, c0:c1], s.at[k], r.at[k], up)

    own_up = rowcopy(xo, 0, width, ro_s, ro_r, 0, False)
    own_dn = rowcopy(xo, 0, width, ro_s, ro_r, 1, True)
    edges, middle = [], []
    for c in range(chunks):
        c0, c1 = xb[c], xb[c + 1]
        edges.append([
            remote(xo.at[:, row, c0:c1], xh.at[:, row, c0:c1], xs_s.at[3 * c + k], xs_r.at[3 * c + k], nxt)
            for k, row in enumerate((1, last))
        ])
        middle.append(
            remote(xo.at[:, 2:last, c0:c1], xh.at[:, 2:last, c0:c1], xs_s.at[3 * c + 2], xs_r.at[3 * c + 2], nxt)
        )
    fwd = [
        (rowcopy(xh, xb[c], xb[c + 1], fw_s, fw_r, 2 * c, False),
         rowcopy(xh, xb[c], xb[c + 1], fw_s, fw_r, 2 * c + 1, True))
        for c in range(chunks)
    ]
    hid = [
        (rowcopy(hs, hb[c], hb[c + 1], he_s, he_r, 2 * c, False),
         rowcopy(hs, hb[c], hb[c + 1], he_s, he_r, 2 * c + 1, True))
        for c in range(chunks)
    ]
    part = [
        remote(ns.at[:, pb[c] : pb[c + 1]], nr.at[:, pb[c] : pb[c + 1]], n_s.at[c], n_r.at[c], nxt)
        for c in range(chunks)
    ]

    @pl.when(has_next)
    def _():
        for pair in edges:
            for copy in pair:
                copy.start()
        for copy in middle:
            copy.start()

    @pl.when(has_up & even)
    def _():
        pl.semaphore_signal(ready.at[0], inc=1, device_id=up, device_id_type=MESH)
        own_up.start()

    @pl.when(has_dn & even)
    def _():
        pl.semaphore_signal(ready.at[1], inc=1, device_id=dn, device_id_type=MESH)
        own_dn.start()

    @pl.when(has_dn & odd)
    def _():
        pl.semaphore_wait(ready.at[0], 1)
        own_dn.start()

    @pl.when(has_up & odd)
    def _():
        pl.semaphore_wait(ready.at[1], 1)
        own_up.start()

    @pl.when(has_dn)
    def _():
        own_up.wait_recv()

    @pl.when(has_up)
    def _():
        own_dn.wait_recv()

    def forward(c):
        @pl.when(has_prev)
        def _():
            for copy in edges[c]:
                copy.wait_recv()

        @pl.when(has_prev & has_up)
        def _():
            fwd[c][0].start()

        @pl.when(has_prev & has_dn)
        def _():
            fwd[c][1].start()

    def own_half(r0, unit0, unit1):
        def left(f, p):
            return lambda: xo[f, r0 + p : r0 + p + 2].reshape(2 * width, chans)

        def pair(accs, q, p):
            return (lambda: w1[2, p, q]), [(accs[0], left(0, p)), (accs[1], left(1, p))]

        def single(accs, q, p):
            return (lambda: w1[1, p, q]), [(accs[1], left(0, p))]

        jobs = first_jobs(unit0, unit1, pair, single)
        matmuls(jobs)
        store_taps(unit0, unit1, lambda v: v.reshape(2, width, chans), slice(r0, r0 + 2), slice(PAD, PAD + width), False)

    def first_jobs(unit0, unit1, pair, single):
        out = []
        for accs, q, extra in ((unit0, 0, ((pair, 0), (single, 0), (single, 1))), (unit1, 2, ((pair, 1), (pair, 2), (single, 2)))):
            job = []
            for p in range(3):
                job += [pair(accs[:2], q, p), single(accs[:2], q, p)]
            out.append(job + [kind(accs[2:], 1, p) for kind, p in extra])
        return out

    def store_taps(unit0, unit1, shape, rws, cols, add):
        for f in range(2):
            parts = (unit0[f], unit0[2 + f], unit1[f], unit1[2 + f])
            zero, one0, two, one1 = (shape(pltpu.matmul_pop(part)) for part in parts)
            for q, value in ((0, zero), (1, one0 + one1), (2, two)):
                if add:
                    acc[q, f, rws, cols, :] += value
                else:
                    acc[q, f, rws, cols, :] = value

    load_w1_own.wait()
    for r0 in (0, 2):
        accumulators(functools.partial(own_half, r0), 2 * width, 4)
    load_w2.wait()
    w01[...] = (w2[0].astype(F32) + w2[1].astype(F32)).astype(BF16)
    load_w1_prev.wait()
    for c in range(chunks):
        forward(c)

    def shifted_sum(ref, c0, c1):
        return sum(ref[q, ..., PAD - 1 + q + c0 : PAD - 1 + q + c1, :] for q in range(3))

    bias1 = b1_ref[...].reshape(1, 1, chans)
    bias2 = b2_ref[...].reshape(1, 1, chans)

    def first_conv(c, unit0, unit1):
        c0, c1 = xb[c], xb[c + 1]
        size = rows * (c1 - c0)

        def left(f, p):
            return lambda: xh[f, p : p + rows, c0:c1].reshape(size, chans)

        def pair(accs, q, p):
            return (lambda: w1[0, p, q]), [(accs[0], left(0, p)), (accs[1], left(1, p))]

        def single(accs, q, p):
            return (lambda: w1[1, p, q]), [(accs[0], left(1, p))]

        @pl.when(has_prev & has_dn)
        def _():
            fwd[c][0].wait_recv()

        @pl.when(has_prev & has_up)
        def _():
            fwd[c][1].wait_recv()

        @pl.when(has_prev)
        def _():
            middle[c].wait_recv()
            matmuls(first_jobs(unit0, unit1, pair, single))
            store_taps(
                unit0, unit1, lambda v: v.reshape(rows, c1 - c0, chans), slice(None), slice(PAD + c0, PAD + c1), True
            )

        h0, h1 = hb[c], hb[c + 1]
        y = [shifted_sum(acc.at[:, f], h0, h1) + bias1 for f in range(2)]
        y = [(v / (1.0 + jnp.exp(-v))).astype(BF16) for v in y]
        hs[0, 1 : rows + 1, h0:h1] = y[0]
        hs[1, 1 : rows + 1, h0:h1] = (y[0].astype(F32) + y[1].astype(F32)).astype(BF16)

        @pl.when(has_up)
        def _():
            hid[c][0].start()

        @pl.when(has_dn)
        def _():
            hid[c][1].start()

    def second_conv(c, unit0, unit1):
        @pl.when(has_dn)
        def _():
            hid[c][0].wait_recv()

        @pl.when(has_up)
        def _():
            hid[c][1].wait_recv()

        h0, h1 = hb[c], hb[c + 1]
        size = rows * (h1 - h0)

        def job(accs, kind, q, p):
            weight = ((lambda: w2[1, p, q]), (lambda: w2[2, p, q]), (lambda: w01[p, q]))[kind]
            return weight, [(accs, lambda: hs[min(kind, 1), p : p + rows, h0:h1].reshape(size, chans))]

        jobs = []
        for accs, q, extra in ((unit0, 0, ((0, 0), (0, 1), (0, 2), (1, 0))), (unit1, 2, ((2, 0), (2, 1), (2, 2), (1, 1), (1, 2)))):
            first = [job(accs[kind], kind, q, p) for kind in range(3) for p in range(3)]
            jobs.append(first + [job(accs[4 if kind == 1 else 3], kind, 1, p) for kind, p in extra])
        matmuls(jobs)
        pops = [[pltpu.matmul_pop(a).reshape(rows, h1 - h0, chans) for a in unit] for unit in (unit0, unit1)]
        (one0, two0, mix0, one1, part0), (one2, two2, mix2, mix1, part1) = pops
        inside = slice(PAD + h0, PAD + h1)
        for q, one, two, mix in ((0, one0, two0, mix0), (1, one1, part0 + part1, mix1), (2, one2, two2, mix2)):
            oq[q, :, inside, :] = one + two
            nq[q, :, inside, :] = mix - one
        p0, p1 = pb[c], pb[c + 1]
        ns[:, p0:p1] = shifted_sum(nq, p0, p1).astype(BF16)

        @pl.when(has_next)
        def _():
            part[c].start()

        own = xo[0, 1 : rows + 1, p0:p1].astype(F32) + xo[1, 1 : rows + 1, p0:p1].astype(F32)
        ob[:, p0:p1] = 0.5 * (shifted_sum(oq, p0, p1) + own) + bias2

    def first(c):
        accumulators(functools.partial(first_conv, c), rows * (xb[c + 1] - xb[c]), 4)

    def second(c):
        accumulators(functools.partial(second_conv, c), rows * (hb[c + 1] - hb[c]), 5)

    first(0)
    for c in range(1, chunks):
        first(c)
        second(c - 1)
    second(chunks - 1)

    for c in range(chunks):
        @pl.when(has_prev)
        def _():
            part[c].wait_recv()

        p0, p1 = pb[c], pb[c + 1]
        out[0, :, p0:p1] = (ob[:, p0:p1] + 0.5 * nr[:, p0:p1].astype(F32)).astype(BF16)

    @pl.when(has_next)
    def _():
        for c in range(chunks):
            for copy in (*edges[c], middle[c], part[c]):
                copy.wait_send()

    @pl.when(has_up)
    def _():
        own_up.wait_send()
        for c in range(chunks):
            hid[c][0].wait_send()

    @pl.when(has_dn)
    def _():
        own_dn.wait_send()
        for c in range(chunks):
            hid[c][1].wait_send()

    @pl.when(has_prev & has_up)
    def _():
        for c in range(chunks):
            fwd[c][0].wait_send()

    @pl.when(has_prev & has_dn)
    def _():
        for c in range(chunks):
            fwd[c][1].wait_send()


def shards(x, w1, b1, w2, b2):
    frames, rows, width, chans = x.shape
    chunks = len(bounds(width)[0]) - 1
    dma = pltpu.SemaphoreType.DMA
    hbm, vmem = pl.BlockSpec(memory_space=pltpu.HBM), pl.BlockSpec(memory_space=pltpu.VMEM)
    extended = pltpu.VMEM((frames, rows + 2, width, chans), BF16)
    taps = pltpu.VMEM((3, rows, width + 2 * PAD, chans), F32)
    flat = pltpu.VMEM((rows, width, chans), BF16)
    return pl.pallas_call(
        kernel,
        out_shape=jax.ShapeDtypeStruct((1, rows, width, chans), BF16),
        in_specs=[hbm, hbm, vmem, hbm, vmem],
        out_specs=vmem,
        scratch_shapes=[
            extended, extended,
            pltpu.VMEM(w1.shape, BF16), pltpu.VMEM(w2.shape, BF16), pltpu.VMEM(w2.shape[1:], BF16),
            pltpu.VMEM((3, frames, rows, width + 2 * PAD, chans), F32),
            extended, taps, taps, pltpu.VMEM((rows, width, chans), F32),
            flat, flat,
            dma((4,)), pltpu.SemaphoreType.REGULAR((2,)),
            dma((3 * chunks,)), dma((3 * chunks,)),
            dma((2,)), dma((2,)),
            dma((2 * chunks,)), dma((2 * chunks,)),
            dma((2 * chunks,)), dma((2 * chunks,)),
            dma((chunks,)), dma((chunks,)),
        ],
        compiler_params=pltpu.CompilerParams(
            collective_id=0, has_side_effects=True, vmem_limit_bytes=67043328
        ),
    )(x, w1, b1.reshape(1, chans), w2, b2.reshape(1, chans))


def solution(mesh):
    spec = P(("clips", "tm"), "tile", None, None)
    return jax.shard_map(shards, mesh=mesh, in_specs=(spec, P(), P(), P(), P()), out_specs=spec, check_vma=False)
```

```python
import functools

import jax
import jax.numpy as jnp
from jax import lax
from jax.experimental import pallas as pl
from jax.experimental.pallas import tpu as pltpu
from jax.sharding import PartitionSpec as P

MESH = pl.DeviceIdType.MESH
PAD = 8
ORDER = ((0, 0), (0, 1), (0, 2), (0, 3), (1, 0), (1, 1), (1, 2), (1, 3))
F32 = jnp.float32
BF16 = jnp.bfloat16


def matmuls(jobs):
    units = range(len(jobs))
    for m in units:
        pltpu.matmul_push_rhs(jobs[m][0][0](), staging_register=0, mxu_index=m)
    for k in range(max(len(job) for job in jobs)):
        for m in units:
            if k + 1 < len(jobs[m]):
                pltpu.matmul_push_rhs(jobs[m][k + 1][0](), staging_register=(k + 1) % 2, mxu_index=m)
        for m in units:
            if k < len(jobs[m]):
                for n, (acc, left) in enumerate(jobs[m][k][1]):
                    pltpu.matmul_acc_lhs(acc, left(), load_staged_rhs=k % 2 if n == 0 else None)


def accumulators(body, size, count):
    spec = [pltpu.ACC(m)((size, 256), F32) for m in (0, 1) for _ in range(count)]
    pl.run_scoped(lambda *accs: body(accs[:count], accs[count:]), *spec)


def bounds(width):
    step = width // 4
    xs = [0, step + 16, 2 * step + 16, 3 * step + 16, width]
    hs = [0, step, 2 * step, 3 * step, width]
    os = [0, step - 16, 2 * step - 16, 3 * step - 16, width]
    return xs, hs, os


def kernel(
    x_hbm, w1_hbm, b1_ref, w2_hbm, b2_ref, out,
    xo, xh, w1, w2, w01, acc, hs, oq, nq, ob, ns, nr,
    ld, ready, xs_s, xs_r, ro_s, ro_r, fw_s, fw_r, he_s, he_r, n_s, n_r,
):
    frames, rows, width, chans = x_hbm.shape
    xb, hb, pb = bounds(width)
    chunks = len(xb) - 1
    i, j = lax.axis_index("tm"), lax.axis_index("tile")
    ni, nj = lax.axis_size("tm"), lax.axis_size("tile")
    has_prev, has_next = i > 0, i < ni - 1
    has_up, has_dn = j > 0, j < nj - 1
    prev, nxt = {"tm": i - 1}, {"tm": i + 1}
    up, dn = {"tile": j - 1}, {"tile": j + 1}
    last = rows

    def local(src, dst, sem):
        return pltpu.make_async_copy(src, dst, sem)

    def remote(src, dst, ssem, rsem, dev):
        return pltpu.make_async_remote_copy(
            src_ref=src, dst_ref=dst, send_sem=ssem, recv_sem=rsem, device_id=dev, device_id_type=MESH
        )

    load_x = local(x_hbm, xo.at[:, 1 : rows + 1], ld.at[0])
    load_w1_own = local(w1_hbm.at[1:3], w1.at[1:3], ld.at[1])
    load_w1_prev = local(w1_hbm.at[0], w1.at[0], ld.at[2])
    load_w2 = local(w2_hbm, w2, ld.at[3])
    load_x.start()
    load_w1_own.start()
    load_w1_prev.start()
    load_w2.start()

    barrier = pltpu.get_barrier_semaphore()
    odd = lax.rem(j, 2) == 1
    even = jnp.logical_not(odd)
    for cond, dev in ((has_prev, prev), (has_up & odd, up), (has_dn & odd, dn)):
        @pl.when(cond)
        def _(dev=dev):
            pl.semaphore_signal(barrier, inc=1, device_id=dev, device_id_type=MESH)

    for buf in (oq, nq):
        for q, at in ((0, 0), (2, PAD + width)):
            buf[q, :, at : at + PAD, :] = jnp.zeros((rows, PAD, chans), F32)
    for q, at in ((0, 0), (2, PAD + width)):
        acc[q, :, :, at : at + PAD, :] = jnp.zeros((frames, rows, PAD, chans), F32)

    @pl.when(jnp.logical_not(has_prev))
    def _():
        nr[...] = jnp.zeros(nr.shape, BF16)

    for cond, row in ((has_up, 0), (has_dn, last + 1)):
        @pl.when(jnp.logical_not(cond))
        def _(row=row):
            zero = jnp.zeros((frames, width, chans), BF16)
            xo[:, row] = zero
            xh[:, row] = zero
            hs[:, row] = zero

    peers = sum(cond.astype(jnp.int32) for cond in (has_next, has_up & even, has_dn & even))

    @pl.when(peers > 0)
    def _():
        pl.semaphore_wait(barrier, peers)

    @pl.when(has_up & even)
    def _():
        pl.semaphore_signal(ready.at[0], inc=1, device_id=up, device_id_type=MESH)

    @pl.when(has_dn & even)
    def _():
        pl.semaphore_signal(ready.at[1], inc=1, device_id=dn, device_id_type=MESH)

    accumulators(lambda unit0, unit1: [pltpu.matmul_pop(a) for a in (*unit0, *unit1)] and None, 1024, 1)
    load_x.wait()

    def rowcopy(buf, c0, c1, s, r, k, down):
        if down:
            return remote(buf.at[:, last, c0:c1], buf.at[:, 0, c0:c1], s.at[k], r.at[k], dn)
        return remote(buf.at[:, 1, c0:c1], buf.at[:, last + 1, c0:c1], s.at[k], r.at[k], up)

    own_up = rowcopy(xo, 0, width, ro_s, ro_r, 0, False)
    own_dn = rowcopy(xo, 0, width, ro_s, ro_r, 1, True)
    edges, middle = [], []
    for c in range(chunks):
        c0, c1 = xb[c], xb[c + 1]
        edges.append([
            remote(xo.at[:, row, c0:c1], xh.at[:, row, c0:c1], xs_s.at[3 * c + k], xs_r.at[3 * c + k], nxt)
            for k, row in enumerate((1, last))
        ])
        middle.append(
            remote(xo.at[:, 2:last, c0:c1], xh.at[:, 2:last, c0:c1], xs_s.at[3 * c + 2], xs_r.at[3 * c + 2], nxt)
        )
    fwd = [
        (rowcopy(xh, xb[c], xb[c + 1], fw_s, fw_r, 2 * c, False),
         rowcopy(xh, xb[c], xb[c + 1], fw_s, fw_r, 2 * c + 1, True))
        for c in range(chunks)
    ]
    hid = [
        (rowcopy(hs, hb[c], hb[c + 1], he_s, he_r, 2 * c, False),
         rowcopy(hs, hb[c], hb[c + 1], he_s, he_r, 2 * c + 1, True))
        for c in range(chunks)
    ]
    part = [
        remote(ns.at[:, pb[c] : pb[c + 1]], nr.at[:, pb[c] : pb[c + 1]], n_s.at[c], n_r.at[c], nxt)
        for c in range(chunks)
    ]

    @pl.when(has_next)
    def _():
        for pair in edges:
            for copy in pair:
                copy.start()
        for copy in middle:
            copy.start()

    @pl.when(has_up & even)
    def _():
        own_up.start()

    @pl.when(has_dn & even)
    def _():
        own_dn.start()

    @pl.when(has_dn & odd)
    def _():
        pl.semaphore_wait(ready.at[0], 1)
        own_dn.start()

    @pl.when(has_up & odd)
    def _():
        pl.semaphore_wait(ready.at[1], 1)
        own_up.start()

    @pl.when(has_dn)
    def _():
        own_up.wait_recv()

    @pl.when(has_up)
    def _():
        own_dn.wait_recv()

    def forward(c):
        @pl.when(has_prev)
        def _():
            for copy in edges[c]:
                copy.wait_recv()

        @pl.when(has_prev & has_up)
        def _():
            fwd[c][0].start()

        @pl.when(has_prev & has_dn)
        def _():
            fwd[c][1].start()

    def own_half(r0, unit0, unit1):
        def left(f, p):
            return lambda: xo[f, r0 + p : r0 + p + 2].reshape(2 * width, chans)

        def pair(accs, q, p):
            return (lambda: w1[2, p, q]), [(accs[0], left(0, p)), (accs[1], left(1, p))]

        def single(accs, q, p):
            return (lambda: w1[1, p, q]), [(accs[1], left(0, p))]

        jobs = first_jobs(unit0, unit1, pair, single)
        matmuls(jobs)
        store_taps(unit0, unit1, lambda v: v.reshape(2, width, chans), slice(r0, r0 + 2), slice(PAD, PAD + width), False)

    def first_jobs(unit0, unit1, pair, single):
        out = []
        for accs, q, extra in ((unit0, 0, ((pair, 0), (single, 0), (single, 1))), (unit1, 2, ((pair, 1), (pair, 2), (single, 2)))):
            job = []
            for p in range(3):
                job += [pair(accs[:2], q, p), single(accs[:2], q, p)]
            out.append(job + [kind(accs[2:], 1, p) for kind, p in extra])
        return out

    def store_taps(unit0, unit1, shape, rws, cols, add):
        for f in range(2):
            parts = (unit0[f], unit0[2 + f], unit1[f], unit1[2 + f])
            zero, one0, two, one1 = (shape(pltpu.matmul_pop(part)) for part in parts)
            for q, value in ((0, zero), (1, one0 + one1), (2, two)):
                if add:
                    acc[q, f, rws, cols, :] += value
                else:
                    acc[q, f, rws, cols, :] = value

    load_w1_own.wait()
    for r0 in (0, 2):
        accumulators(functools.partial(own_half, r0), 2 * width, 4)
    load_w2.wait()
    w01[...] = w2[0] + w2[1]
    load_w1_prev.wait()
    for c in range(chunks):
        forward(c)

    def shifted_sum(ref, c0, c1):
        return sum(ref[q, ..., PAD - 1 + q + c0 : PAD - 1 + q + c1, :] for q in range(3))

    bias1 = b1_ref[...].reshape(1, 1, chans)
    bias2 = b2_ref[...].reshape(1, 1, chans)

    def first_conv(c, unit0, unit1):
        c0, c1 = xb[c], xb[c + 1]
        size = rows * (c1 - c0)

        def left(f, p):
            return lambda: xh[f, p : p + rows, c0:c1].reshape(size, chans)

        def pair(accs, q, p):
            return (lambda: w1[0, p, q]), [(accs[0], left(0, p)), (accs[1], left(1, p))]

        def single(accs, q, p):
            return (lambda: w1[1, p, q]), [(accs[0], left(1, p))]

        @pl.when(has_prev & has_dn)
        def _():
            fwd[c][0].wait_recv()

        @pl.when(has_prev & has_up)
        def _():
            fwd[c][1].wait_recv()

        @pl.when(has_prev)
        def _():
            middle[c].wait_recv()
            matmuls(first_jobs(unit0, unit1, pair, single))
            store_taps(
                unit0, unit1, lambda v: v.reshape(rows, c1 - c0, chans), slice(None), slice(PAD + c0, PAD + c1), True
            )

        h0, h1 = hb[c], hb[c + 1]
        y = [0.5 * (shifted_sum(acc.at[:, f], h0, h1) + bias1) for f in range(2)]
        y = [(v + v * jnp.tanh(v)).astype(BF16) for v in y]
        hs[0, 1 : rows + 1, h0:h1] = y[0]
        hs[1, 1 : rows + 1, h0:h1] = (y[0].astype(F32) + y[1].astype(F32)).astype(BF16)

        @pl.when(has_up)
        def _():
            hid[c][0].start()

        @pl.when(has_dn)
        def _():
            hid[c][1].start()

    def second_conv(c, unit0, unit1):
        @pl.when(has_dn)
        def _():
            hid[c][0].wait_recv()

        @pl.when(has_up)
        def _():
            hid[c][1].wait_recv()

        h0, h1 = hb[c], hb[c + 1]
        size = rows * (h1 - h0)

        def job(accs, kind, q, p):
            weight = ((lambda: w2[1, p, q]), (lambda: w2[2, p, q]), (lambda: w01[p, q]))[kind]
            return weight, [(accs, lambda: hs[min(kind, 1), p : p + rows, h0:h1].reshape(size, chans))]

        jobs = []
        for accs, q, extra in ((unit0, 0, ((0, 0), (0, 1), (0, 2), (1, 0))), (unit1, 2, ((2, 0), (2, 1), (2, 2), (1, 1), (1, 2)))):
            first = [job(accs[kind], kind, q, p) for kind in range(3) for p in range(3)]
            jobs.append(first + [job(accs[4 if kind == 1 else 3], kind, 1, p) for kind, p in extra])
        matmuls(jobs)
        pops = [[pltpu.matmul_pop(a).reshape(rows, h1 - h0, chans) for a in unit] for unit in (unit0, unit1)]
        (one0, two0, mix0, one1, part0), (one2, two2, mix2, mix1, part1) = pops
        inside = slice(PAD + h0, PAD + h1)
        for q, one, two, mix in ((0, one0, two0, mix0), (1, one1, part0 + part1, mix1), (2, one2, two2, mix2)):
            oq[q, :, inside, :] = one + two
            nq[q, :, inside, :] = mix - one
        p0, p1 = pb[c], pb[c + 1]
        ns[:, p0:p1] = shifted_sum(nq, p0, p1).astype(BF16)

        @pl.when(has_next)
        def _():
            part[c].start()

        own = xo[0, 1 : rows + 1, p0:p1].astype(F32) + xo[1, 1 : rows + 1, p0:p1].astype(F32)
        ob[:, p0:p1] = 0.5 * (shifted_sum(oq, p0, p1) + own) + bias2

    def first(c):
        accumulators(functools.partial(first_conv, c), rows * (xb[c + 1] - xb[c]), 4)

    def second(c):
        accumulators(functools.partial(second_conv, c), rows * (hb[c + 1] - hb[c]), 5)

    for stage, c in ORDER:
        (first, second)[stage](c)

    for c in range(chunks):
        @pl.when(has_prev)
        def _():
            part[c].wait_recv()

        p0, p1 = pb[c], pb[c + 1]
        out[0, :, p0:p1] = (ob[:, p0:p1] + 0.5 * nr[:, p0:p1].astype(F32)).astype(BF16)

    @pl.when(has_next)
    def _():
        for c in range(chunks):
            for copy in (*edges[c], middle[c], part[c]):
                copy.wait_send()

    @pl.when(has_up)
    def _():
        own_up.wait_send()
        for c in range(chunks):
            hid[c][0].wait_send()

    @pl.when(has_dn)
    def _():
        own_dn.wait_send()
        for c in range(chunks):
            hid[c][1].wait_send()

    @pl.when(has_prev & has_up)
    def _():
        for c in range(chunks):
            fwd[c][0].wait_send()

    @pl.when(has_prev & has_dn)
    def _():
        for c in range(chunks):
            fwd[c][1].wait_send()


def shards(x, w1, b1, w2, b2):
    frames, rows, width, chans = x.shape
    chunks = len(bounds(width)[0]) - 1
    dma = pltpu.SemaphoreType.DMA
    hbm, vmem = pl.BlockSpec(memory_space=pltpu.HBM), pl.BlockSpec(memory_space=pltpu.VMEM)
    extended = pltpu.VMEM((frames, rows + 2, width, chans), BF16)
    taps = pltpu.VMEM((3, rows, width + 2 * PAD, chans), F32)
    flat = pltpu.VMEM((rows, width, chans), BF16)
    return pl.pallas_call(
        kernel,
        out_shape=pltpu.VMEM((1, rows, width, chans), BF16),
        in_specs=[hbm, hbm, vmem, hbm, vmem],
        out_specs=vmem,
        scratch_shapes=[
            extended, extended,
            pltpu.VMEM(w1.shape, BF16), pltpu.VMEM(w2.shape, BF16), pltpu.VMEM(w2.shape[1:], BF16),
            pltpu.VMEM((3, frames, rows, width + 2 * PAD, chans), F32),
            extended, taps, taps, pltpu.VMEM((rows, width, chans), F32),
            flat, flat,
            dma((4,)), pltpu.SemaphoreType.REGULAR((2,)),
            dma((3 * chunks,)), dma((3 * chunks,)),
            dma((2,)), dma((2,)),
            dma((2 * chunks,)), dma((2 * chunks,)),
            dma((2 * chunks,)), dma((2 * chunks,)),
            dma((chunks,)), dma((chunks,)),
        ],
        compiler_params=pltpu.CompilerParams(
            collective_id=0, has_side_effects=True, vmem_limit_bytes=67043328 - 600000
        ),
    )(x, w1, b1.reshape(1, chans), w2, b2.reshape(1, chans))


def solution(mesh):
    spec = P(("clips", "tm"), "tile", None, None)
    return jax.shard_map(shards, mesh=mesh, in_specs=(spec, P(), P(), P(), P()), out_specs=spec, check_vma=False)
```

```python
import functools

import jax
import jax.numpy as jnp
from jax import lax
from jax.experimental import pallas as pl
from jax.experimental.pallas import tpu as pltpu
from jax.sharding import PartitionSpec as P

MESH = pl.DeviceIdType.MESH
PAD = 8
ORDER = ((0, 0), (0, 1), (0, 2), (0, 3), (1, 0), (1, 1), (1, 2), (1, 3), (2, 0), (2, 1), (2, 2), (2, 3))
F32 = jnp.float32
BF16 = jnp.bfloat16


def matmuls(jobs):
    units = range(len(jobs))
    for m in units:
        pltpu.matmul_push_rhs(jobs[m][0][0](), staging_register=0, mxu_index=m)
    for k in range(max(len(job) for job in jobs)):
        for m in units:
            if k + 1 < len(jobs[m]):
                pltpu.matmul_push_rhs(jobs[m][k + 1][0](), staging_register=(k + 1) % 2, mxu_index=m)
        for m in units:
            if k < len(jobs[m]):
                for n, (acc, left) in enumerate(jobs[m][k][1]):
                    pltpu.matmul_acc_lhs(acc, left(), load_staged_rhs=k % 2 if n == 0 else None)


def accumulators(body, size, count):
    spec = [pltpu.ACC(m)((size, 256), F32) for m in (0, 1) for _ in range(count)]
    pl.run_scoped(lambda *accs: body(accs[:count], accs[count:]), *spec)


def bounds(width):
    step = width // 4
    xs = [0, step + 16, 2 * step + 16, 3 * step + 16, width]
    hs = [0, step, 2 * step, 3 * step, width]
    os = [0, step - 16, 2 * step - 16, 3 * step - 16, width]
    return xs, hs, os


def kernel(
    x_hbm, w1_hbm, b1_hbm, w2_hbm, b2_hbm, out,
    xo, xh, w1, w2, w01, b1_ref, b2_ref, acc, hs, oq, nq, ob, ns, nr,
    ld, ready, xs_s, xs_r, ro_s, ro_r, fw_s, fw_r, he_s, he_r, n_s, n_r,
):
    frames, rows, width, chans = x_hbm.shape
    xb, hb, pb = bounds(width)
    chunks = len(xb) - 1
    i, j = lax.axis_index("tm"), lax.axis_index("tile")
    ni, nj = lax.axis_size("tm"), lax.axis_size("tile")
    has_prev, has_next = i > 0, i < ni - 1
    has_up, has_dn = j > 0, j < nj - 1
    prev, nxt = {"tm": i - 1}, {"tm": i + 1}
    up, dn = {"tile": j - 1}, {"tile": j + 1}
    last = rows

    def local(src, dst, sem):
        return pltpu.make_async_copy(src, dst, sem)

    def remote(src, dst, ssem, rsem, dev):
        return pltpu.make_async_remote_copy(
            src_ref=src, dst_ref=dst, send_sem=ssem, recv_sem=rsem, device_id=dev, device_id_type=MESH
        )

    load_x = local(x_hbm, xo.at[:, 1 : rows + 1], ld.at[0])
    load_w1_own = local(w1_hbm.at[1:3], w1.at[1:3], ld.at[1])
    load_w1_prev = local(w1_hbm.at[0], w1.at[0], ld.at[2])
    load_w2 = local(w2_hbm, w2, ld.at[3])
    load_b1 = local(b1_hbm, b1_ref, ld.at[4])
    load_b2 = local(b2_hbm, b2_ref, ld.at[5])
    load_x.start()

    barrier = pltpu.get_barrier_semaphore()
    odd = lax.rem(j, 2) == 1
    even = jnp.logical_not(odd)
    for cond, dev in ((has_prev, prev), (has_up & odd, up), (has_dn & odd, dn)):
        @pl.when(cond)
        def _(dev=dev):
            pl.semaphore_signal(barrier, inc=1, device_id=dev, device_id_type=MESH)

    peers = sum(cond.astype(jnp.int32) for cond in (has_next, has_up & even, has_dn & even))

    @pl.when(peers > 0)
    def _():
        pl.semaphore_wait(barrier, peers)

    @pl.when(has_up & even)
    def _():
        pl.semaphore_signal(ready.at[0], inc=1, device_id=up, device_id_type=MESH)

    @pl.when(has_dn & even)
    def _():
        pl.semaphore_signal(ready.at[1], inc=1, device_id=dn, device_id_type=MESH)

    load_x.wait()

    def rowcopy(buf, c0, c1, s, r, k, down):
        if down:
            return remote(buf.at[:, last, c0:c1], buf.at[:, 0, c0:c1], s.at[k], r.at[k], dn)
        return remote(buf.at[:, 1, c0:c1], buf.at[:, last + 1, c0:c1], s.at[k], r.at[k], up)

    own_up = rowcopy(xo, 0, width, ro_s, ro_r, 0, False)
    own_dn = rowcopy(xo, 0, width, ro_s, ro_r, 1, True)
    edges, middle = [], []
    for c in range(chunks):
        c0, c1 = xb[c], xb[c + 1]
        edges.append([
            remote(xo.at[:, row, c0:c1], xh.at[:, row, c0:c1], xs_s.at[3 * c + k], xs_r.at[3 * c + k], nxt)
            for k, row in enumerate((1, last))
        ])
        middle.append(
            remote(xo.at[:, 2:last, c0:c1], xh.at[:, 2:last, c0:c1], xs_s.at[3 * c + 2], xs_r.at[3 * c + 2], nxt)
        )
    fwd = [
        (rowcopy(xh, xb[c], xb[c + 1], fw_s, fw_r, 2 * c, False),
         rowcopy(xh, xb[c], xb[c + 1], fw_s, fw_r, 2 * c + 1, True))
        for c in range(chunks)
    ]
    hid = [
        (rowcopy(hs, hb[c], hb[c + 1], he_s, he_r, 2 * c, False),
         rowcopy(hs, hb[c], hb[c + 1], he_s, he_r, 2 * c + 1, True))
        for c in range(chunks)
    ]
    part = [
        remote(ns.at[:, pb[c] : pb[c + 1]], nr.at[:, pb[c] : pb[c + 1]], n_s.at[c], n_r.at[c], nxt)
        for c in range(chunks)
    ]

    @pl.when(has_next)
    def _():
        for pair in edges:
            for copy in pair:
                copy.start()
        for copy in middle:
            copy.start()

    @pl.when(has_up & even)
    def _():
        own_up.start()

    @pl.when(has_dn & even)
    def _():
        own_dn.start()

    load_w1_own.start()
    load_w1_prev.start()
    load_w2.start()
    load_b1.start()
    load_b2.start()
    accumulators(lambda unit0, unit1: [pltpu.matmul_pop(a) for a in (*unit0, *unit1)] and None, 1024, 1)

    for buf in (oq, nq):
        for q, at in ((0, 0), (2, PAD + width)):
            buf[q, :, at : at + PAD, :] = jnp.zeros((rows, PAD, chans), F32)
    for q, at in ((0, 0), (2, PAD + width)):
        acc[q, :, :, at : at + PAD, :] = jnp.zeros((frames, rows, PAD, chans), F32)

    @pl.when(jnp.logical_not(has_prev))
    def _():
        nr[...] = jnp.zeros(nr.shape, BF16)

    for cond, row in ((has_up, 0), (has_dn, last + 1)):
        @pl.when(jnp.logical_not(cond))
        def _(row=row):
            zero = jnp.zeros((frames, width, chans), BF16)
            xo[:, row] = zero
            xh[:, row] = zero
            hs[:, row] = zero

    @pl.when(has_dn & odd)
    def _():
        pl.semaphore_wait(ready.at[0], 1)
        own_dn.start()

    @pl.when(has_up & odd)
    def _():
        pl.semaphore_wait(ready.at[1], 1)
        own_up.start()

    @pl.when(has_dn)
    def _():
        own_up.wait_recv()

    @pl.when(has_up)
    def _():
        own_dn.wait_recv()

    def forward(c):
        @pl.when(has_prev)
        def _():
            for copy in edges[c]:
                copy.wait_recv()

        @pl.when(has_prev & has_up)
        def _():
            fwd[c][0].start()

        @pl.when(has_prev & has_dn)
        def _():
            fwd[c][1].start()

    def own_half(r0, unit0, unit1):
        def left(f, p):
            return lambda: xo[f, r0 + p : r0 + p + 2].reshape(2 * width, chans)

        def pair(accs, q, p):
            return (lambda: w1[2, p, q]), [(accs[0], left(0, p)), (accs[1], left(1, p))]

        def single(accs, q, p):
            return (lambda: w1[1, p, q]), [(accs[1], left(0, p))]

        jobs = first_jobs(unit0, unit1, pair, single)
        matmuls(jobs)
        store_taps(unit0, unit1, lambda v: v.reshape(2, width, chans), slice(r0, r0 + 2), slice(PAD, PAD + width), False)

    def first_jobs(unit0, unit1, pair, single):
        out = []
        for accs, q, extra in ((unit0, 0, ((pair, 0), (single, 0), (single, 1))), (unit1, 2, ((pair, 1), (pair, 2), (single, 2)))):
            job = []
            for p in range(3):
                job += [pair(accs[:2], q, p), single(accs[:2], q, p)]
            out.append(job + [kind(accs[2:], 1, p) for kind, p in extra])
        return out

    def store_taps(unit0, unit1, shape, rws, cols, add):
        for f in range(2):
            parts = (unit0[f], unit0[2 + f], unit1[f], unit1[2 + f])
            zero, one0, two, one1 = (shape(pltpu.matmul_pop(part)) for part in parts)
            for q, value in ((0, zero), (1, one0 + one1), (2, two)):
                if add:
                    acc[q, f, rws, cols, :] += value
                else:
                    acc[q, f, rws, cols, :] = value

    load_w1_own.wait()
    for r0 in (0, 2):
        accumulators(functools.partial(own_half, r0), 2 * width, 4)
    load_w2.wait()
    w01[...] = w2[0] + w2[1]
    load_w1_prev.wait()
    load_b1.wait()
    load_b2.wait()
    def shifted_sum(ref, c0, c1):
        return sum(ref[q, ..., PAD - 1 + q + c0 : PAD - 1 + q + c1, :] for q in range(3))

    bias1 = b1_ref[...].reshape(1, 1, chans)
    bias2 = b2_ref[...].reshape(1, 1, chans)

    def first_conv(c, unit0, unit1):
        c0, c1 = xb[c], xb[c + 1]
        size = rows * (c1 - c0)

        def left(f, p):
            return lambda: xh[f, p : p + rows, c0:c1].reshape(size, chans)

        def pair(accs, q, p):
            return (lambda: w1[0, p, q]), [(accs[0], left(0, p)), (accs[1], left(1, p))]

        def single(accs, q, p):
            return (lambda: w1[1, p, q]), [(accs[0], left(1, p))]

        @pl.when(has_prev & has_dn)
        def _():
            fwd[c][0].wait_recv()

        @pl.when(has_prev & has_up)
        def _():
            fwd[c][1].wait_recv()

        @pl.when(has_prev)
        def _():
            middle[c].wait_recv()
            matmuls(first_jobs(unit0, unit1, pair, single))
            store_taps(
                unit0, unit1, lambda v: v.reshape(rows, c1 - c0, chans), slice(None), slice(PAD + c0, PAD + c1), True
            )

        h0, h1 = hb[c], hb[c + 1]
        y = [0.5 * (shifted_sum(acc.at[:, f], h0, h1) + bias1) for f in range(2)]
        y = [(v + v * jnp.tanh(v)).astype(BF16) for v in y]
        hs[0, 1 : rows + 1, h0:h1] = y[0]
        hs[1, 1 : rows + 1, h0:h1] = (y[0].astype(F32) + y[1].astype(F32)).astype(BF16)

        @pl.when(has_up)
        def _():
            hid[c][0].start()

        @pl.when(has_dn)
        def _():
            hid[c][1].start()

    def second_conv(c, unit0, unit1):
        @pl.when(has_dn)
        def _():
            hid[c][0].wait_recv()

        @pl.when(has_up)
        def _():
            hid[c][1].wait_recv()

        h0, h1 = hb[c], hb[c + 1]
        size = rows * (h1 - h0)

        def job(accs, kind, q, p):
            weight = ((lambda: w2[1, p, q]), (lambda: w2[2, p, q]), (lambda: w01[p, q]))[kind]
            return weight, [(accs, lambda: hs[min(kind, 1), p : p + rows, h0:h1].reshape(size, chans))]

        jobs = []
        for accs, q, extra in ((unit0, 0, ((0, 0), (0, 1), (0, 2), (1, 0))), (unit1, 2, ((2, 0), (2, 1), (2, 2), (1, 1), (1, 2)))):
            first = [job(accs[kind], kind, q, p) for kind in range(3) for p in range(3)]
            jobs.append(first + [job(accs[4 if kind == 1 else 3], kind, 1, p) for kind, p in extra])
        matmuls(jobs)
        pops = [[pltpu.matmul_pop(a).reshape(rows, h1 - h0, chans) for a in unit] for unit in (unit0, unit1)]
        (one0, two0, mix0, one1, part0), (one2, two2, mix2, mix1, part1) = pops
        inside = slice(PAD + h0, PAD + h1)
        for q, one, two, mix in ((0, one0, two0, mix0), (1, one1, part0 + part1, mix1), (2, one2, two2, mix2)):
            oq[q, :, inside, :] = one + two
            nq[q, :, inside, :] = mix - one
        p0, p1 = pb[c], pb[c + 1]
        ns[:, p0:p1] = shifted_sum(nq, p0, p1).astype(BF16)

        @pl.when(has_next)
        def _():
            part[c].start()

        own = xo[0, 1 : rows + 1, p0:p1].astype(F32) + xo[1, 1 : rows + 1, p0:p1].astype(F32)
        ob[:, p0:p1] = 0.5 * (shifted_sum(oq, p0, p1) + own) + bias2

    def first(c):
        accumulators(functools.partial(first_conv, c), rows * (xb[c + 1] - xb[c]), 4)

    def second(c):
        accumulators(functools.partial(second_conv, c), rows * (hb[c + 1] - hb[c]), 5)

    for stage, c in ORDER:
        (forward, first, second)[stage](c)

    for c in range(chunks):
        @pl.when(has_prev)
        def _():
            part[c].wait_recv()

        p0, p1 = pb[c], pb[c + 1]
        out[0, :, p0:p1] = (ob[:, p0:p1] + 0.5 * nr[:, p0:p1].astype(F32)).astype(BF16)

    @pl.when(has_next)
    def _():
        for c in range(chunks):
            for copy in (*edges[c], middle[c], part[c]):
                copy.wait_send()

    @pl.when(has_up)
    def _():
        own_up.wait_send()
        for c in range(chunks):
            hid[c][0].wait_send()

    @pl.when(has_dn)
    def _():
        own_dn.wait_send()
        for c in range(chunks):
            hid[c][1].wait_send()

    @pl.when(has_prev & has_up)
    def _():
        for c in range(chunks):
            fwd[c][0].wait_send()

    @pl.when(has_prev & has_dn)
    def _():
        for c in range(chunks):
            fwd[c][1].wait_send()


def shards(x, w1, b1, w2, b2):
    frames, rows, width, chans = x.shape
    chunks = len(bounds(width)[0]) - 1
    dma = pltpu.SemaphoreType.DMA
    hbm, vmem = pl.BlockSpec(memory_space=pltpu.HBM), pl.BlockSpec(memory_space=pltpu.VMEM)
    extended = pltpu.VMEM((frames, rows + 2, width, chans), BF16)
    taps = pltpu.VMEM((3, rows, width + 2 * PAD, chans), F32)
    flat = pltpu.VMEM((rows, width, chans), BF16)
    return pl.pallas_call(
        kernel,
        out_shape=pltpu.VMEM((1, rows, width, chans), BF16),
        in_specs=[hbm] * 5,
        out_specs=vmem,
        scratch_shapes=[
            extended, extended,
            pltpu.VMEM(w1.shape, BF16), pltpu.VMEM(w2.shape, BF16), pltpu.VMEM(w2.shape[1:], BF16),
            pltpu.VMEM((1, chans), F32), pltpu.VMEM((1, chans), F32),
            pltpu.VMEM((3, frames, rows, width + 2 * PAD, chans), F32),
            extended, taps, taps, pltpu.VMEM((rows, width, chans), F32),
            flat, flat,
            dma((6,)), pltpu.SemaphoreType.REGULAR((2,)),
            dma((3 * chunks,)), dma((3 * chunks,)),
            dma((2,)), dma((2,)),
            dma((2 * chunks,)), dma((2 * chunks,)),
            dma((2 * chunks,)), dma((2 * chunks,)),
            dma((chunks,)), dma((chunks,)),
        ],
        compiler_params=pltpu.CompilerParams(
            collective_id=0, has_side_effects=True, vmem_limit_bytes=67043328 - 600000
        ),
    )(x, w1, b1.reshape(1, chans), w2, b2.reshape(1, chans))


def solution(mesh):
    spec = P(("clips", "tm"), "tile", None, None)
    return jax.shard_map(shards, mesh=mesh, in_specs=(spec, P(), P(), P(), P()), out_specs=spec, check_vma=False)
```

```python
import functools

import jax
import jax.numpy as jnp
from jax import lax
from jax.experimental import pallas as pl
from jax.experimental.pallas import tpu as pltpu
from jax.sharding import PartitionSpec as P

MESH = pl.DeviceIdType.MESH
PAD = 8
ORDER = ((0, 0), (0, 1), (0, 2), (1, 0), (1, 1), (1, 2), (2, 0), (2, 1), (2, 2), (2, 3))
F32 = jnp.float32
BF16 = jnp.bfloat16


def matmuls(jobs):
    units = range(len(jobs))
    for m in units:
        pltpu.matmul_push_rhs(jobs[m][0][0](), staging_register=0, mxu_index=m)
    for k in range(max(len(job) for job in jobs)):
        for m in units:
            if k + 1 < len(jobs[m]):
                pltpu.matmul_push_rhs(jobs[m][k + 1][0](), staging_register=(k + 1) % 2, mxu_index=m)
        for m in units:
            if k < len(jobs[m]):
                for n, (acc, left) in enumerate(jobs[m][k][1]):
                    pltpu.matmul_acc_lhs(acc, left(), load_staged_rhs=k % 2 if n == 0 else None)


def accumulators(body, size, count):
    spec = [pltpu.ACC(m)((size, 256), F32) for m in (0, 1) for _ in range(count)]
    pl.run_scoped(lambda *accs: body(accs[:count], accs[count:]), *spec)


def bounds(width):
    step = width // 4
    xs = [0, step + 16, 2 * step + 16, width]
    hs = [0, step, 2 * step, width]
    ss = [0, step, 2 * step, 3 * step, width]
    ps = [0, step - 16, 2 * step - 16, 3 * step - 16, width]
    return xs, hs, ss, ps


def kernel(
    x_hbm, w1_hbm, b1_hbm, w2_hbm, b2_hbm, out,
    xo, xh, w1, w2, w01, b1_ref, b2_ref, acc, hs, oq, nq, ob, ns, nr,
    ld, ready, xs_s, xs_r, ro_s, ro_r, fw_s, fw_r, he_s, he_r, n_s, n_r,
):
    frames, rows, width, chans = x_hbm.shape
    xb, hb, sb, pb = bounds(width)
    chunks, pieces = len(xb) - 1, len(pb) - 1
    i, j = lax.axis_index("tm"), lax.axis_index("tile")
    ni, nj = lax.axis_size("tm"), lax.axis_size("tile")
    has_prev, has_next = i > 0, i < ni - 1
    has_up, has_dn = j > 0, j < nj - 1
    prev, nxt = {"tm": i - 1}, {"tm": i + 1}
    up, dn = {"tile": j - 1}, {"tile": j + 1}
    last = rows

    def local(src, dst, sem):
        return pltpu.make_async_copy(src, dst, sem)

    def remote(src, dst, ssem, rsem, dev):
        return pltpu.make_async_remote_copy(
            src_ref=src, dst_ref=dst, send_sem=ssem, recv_sem=rsem, device_id=dev, device_id_type=MESH
        )

    load_x = [
        local(x_hbm.at[:, a:b], xo.at[:, a + 1 : b + 1], ld.at[k])
        for k, a, b in ((0, 0, 1), (6, rows - 1, rows), (7, 1, rows - 1))
    ]
    load_w1_own = local(w1_hbm.at[1:3], w1.at[1:3], ld.at[1])
    load_w1_prev = local(w1_hbm.at[0], w1.at[0], ld.at[2])
    load_w2 = local(w2_hbm, w2, ld.at[3])
    load_b1 = local(b1_hbm, b1_ref, ld.at[4])
    load_b2 = local(b2_hbm, b2_ref, ld.at[5])
    for load in load_x:
        load.start()

    barrier = pltpu.get_barrier_semaphore()
    odd = lax.rem(j, 2) == 1
    even = jnp.logical_not(odd)
    for cond, dev in ((has_prev, prev), (has_up & odd, up), (has_dn & odd, dn)):
        @pl.when(cond)
        def _(dev=dev):
            pl.semaphore_signal(barrier, inc=1, device_id=dev, device_id_type=MESH)

    peers = sum(cond.astype(jnp.int32) for cond in (has_next, has_up & even, has_dn & even))

    @pl.when(peers > 0)
    def _():
        pl.semaphore_wait(barrier, peers)

    @pl.when(has_up & even)
    def _():
        pl.semaphore_signal(ready.at[0], inc=1, device_id=up, device_id_type=MESH)

    @pl.when(has_dn & even)
    def _():
        pl.semaphore_signal(ready.at[1], inc=1, device_id=dn, device_id_type=MESH)

    for load in load_x[:2]:
        load.wait()

    def rowcopy(buf, c0, c1, s, r, k, down):
        if down:
            return remote(buf.at[:, last, c0:c1], buf.at[:, 0, c0:c1], s.at[k], r.at[k], dn)
        return remote(buf.at[:, 1, c0:c1], buf.at[:, last + 1, c0:c1], s.at[k], r.at[k], up)

    own_up = rowcopy(xo, 0, width, ro_s, ro_r, 0, False)
    own_dn = rowcopy(xo, 0, width, ro_s, ro_r, 1, True)
    edges, middle = [], []
    for c in range(chunks):
        c0, c1 = xb[c], xb[c + 1]
        edges.append([
            remote(xo.at[:, row, c0:c1], xh.at[:, row, c0:c1], xs_s.at[3 * c + k], xs_r.at[3 * c + k], nxt)
            for k, row in enumerate((1, last))
        ])
        middle.append(
            remote(xo.at[:, 2:last, c0:c1], xh.at[:, 2:last, c0:c1], xs_s.at[3 * c + 2], xs_r.at[3 * c + 2], nxt)
        )
    fwd = [
        (rowcopy(xh, xb[c], xb[c + 1], fw_s, fw_r, 2 * c, False),
         rowcopy(xh, xb[c], xb[c + 1], fw_s, fw_r, 2 * c + 1, True))
        for c in range(chunks)
    ]
    hid = [
        (rowcopy(hs, hb[c], hb[c + 1], he_s, he_r, 2 * c, False),
         rowcopy(hs, hb[c], hb[c + 1], he_s, he_r, 2 * c + 1, True))
        for c in range(chunks)
    ]
    part = [
        remote(ns.at[:, pb[c] : pb[c + 1]], nr.at[:, pb[c] : pb[c + 1]], n_s.at[c], n_r.at[c], nxt)
        for c in range(pieces)
    ]

    @pl.when(has_next)
    def _():
        for pair in edges:
            for copy in pair:
                copy.start()

    load_x[2].wait()

    @pl.when(has_next)
    def _():
        for copy in middle:
            copy.start()

    @pl.when(has_up & even)
    def _():
        own_up.start()

    @pl.when(has_dn & even)
    def _():
        own_dn.start()

    load_w1_own.start()
    load_w1_prev.start()
    load_w2.start()
    load_b1.start()
    load_b2.start()
    accumulators(lambda unit0, unit1: [pltpu.matmul_pop(a) for a in (*unit0, *unit1)] and None, 1024, 1)

    for buf in (oq, nq):
        for q, at in ((0, 0), (2, PAD + width)):
            buf[q, :, at : at + PAD, :] = jnp.zeros((rows, PAD, chans), F32)
    for q, at in ((0, 0), (2, PAD + width)):
        acc[q, :, :, at : at + PAD, :] = jnp.zeros((frames, rows, PAD, chans), F32)

    @pl.when(jnp.logical_not(has_prev))
    def _():
        nr[...] = jnp.zeros(nr.shape, BF16)

    for cond, row in ((has_up, 0), (has_dn, last + 1)):
        @pl.when(jnp.logical_not(cond))
        def _(row=row):
            zero = jnp.zeros((frames, width, chans), BF16)
            xo[:, row] = zero
            xh[:, row] = zero
            hs[:, row] = zero

    @pl.when(has_dn & odd)
    def _():
        pl.semaphore_wait(ready.at[0], 1)
        own_dn.start()

    @pl.when(has_up & odd)
    def _():
        pl.semaphore_wait(ready.at[1], 1)
        own_up.start()

    @pl.when(has_dn)
    def _():
        own_up.wait_recv()

    @pl.when(has_up)
    def _():
        own_dn.wait_recv()

    def forward(c):
        @pl.when(has_prev)
        def _():
            for copy in edges[c]:
                copy.wait_recv()

        @pl.when(has_prev & has_up)
        def _():
            fwd[c][0].start()

        @pl.when(has_prev & has_dn)
        def _():
            fwd[c][1].start()

    def own_half(r0, unit0, unit1):
        def left(f, p):
            return lambda: xo[f, r0 + p : r0 + p + 2].reshape(2 * width, chans)

        def pair(accs, q, p):
            return (lambda: w1[2, p, q]), [(accs[0], left(0, p)), (accs[1], left(1, p))]

        def single(accs, q, p):
            return (lambda: w1[1, p, q]), [(accs[1], left(0, p))]

        jobs = first_jobs(unit0, unit1, pair, single)
        matmuls(jobs)
        store_taps(unit0, unit1, lambda v: v.reshape(2, width, chans), slice(r0, r0 + 2), slice(PAD, PAD + width), False)

    def first_jobs(unit0, unit1, pair, single):
        out = []
        for accs, q, extra in ((unit0, 0, ((pair, 0), (single, 0), (single, 1))), (unit1, 2, ((pair, 1), (pair, 2), (single, 2)))):
            job = []
            for p in range(3):
                job += [pair(accs[:2], q, p), single(accs[:2], q, p)]
            out.append(job + [kind(accs[2:], 1, p) for kind, p in extra])
        return out

    def store_taps(unit0, unit1, shape, rws, cols, add):
        for f in range(2):
            parts = (unit0[f], unit0[2 + f], unit1[f], unit1[2 + f])
            zero, one0, two, one1 = (shape(pltpu.matmul_pop(part)) for part in parts)
            for q, value in ((0, zero), (1, one0 + one1), (2, two)):
                if add:
                    acc[q, f, rws, cols, :] += value
                else:
                    acc[q, f, rws, cols, :] = value

    load_w1_own.wait()
    for r0 in (0, 2):
        accumulators(functools.partial(own_half, r0), 2 * width, 4)
    load_w2.wait()
    w01[...] = w2[0] + w2[1]
    load_w1_prev.wait()
    load_b1.wait()
    load_b2.wait()
    def shifted_sum(ref, c0, c1):
        return sum(ref[q, ..., PAD - 1 + q + c0 : PAD - 1 + q + c1, :] for q in range(3))

    bias1 = b1_ref[...].reshape(1, 1, chans)
    bias2 = b2_ref[...].reshape(1, 1, chans)

    def first_conv(c, unit0, unit1):
        c0, c1 = xb[c], xb[c + 1]
        size = rows * (c1 - c0)

        def left(f, p):
            return lambda: xh[f, p : p + rows, c0:c1].reshape(size, chans)

        def pair(accs, q, p):
            return (lambda: w1[0, p, q]), [(accs[0], left(0, p)), (accs[1], left(1, p))]

        def single(accs, q, p):
            return (lambda: w1[1, p, q]), [(accs[0], left(1, p))]

        @pl.when(has_prev & has_dn)
        def _():
            fwd[c][0].wait_recv()

        @pl.when(has_prev & has_up)
        def _():
            fwd[c][1].wait_recv()

        @pl.when(has_prev)
        def _():
            middle[c].wait_recv()
            matmuls(first_jobs(unit0, unit1, pair, single))
            store_taps(
                unit0, unit1, lambda v: v.reshape(rows, c1 - c0, chans), slice(None), slice(PAD + c0, PAD + c1), True
            )

        h0, h1 = hb[c], hb[c + 1]
        y = [0.5 * (shifted_sum(acc.at[:, f], h0, h1) + bias1) for f in range(2)]
        y = [(v + v * jnp.tanh(v)).astype(BF16) for v in y]
        hs[0, 1 : rows + 1, h0:h1] = y[0]
        hs[1, 1 : rows + 1, h0:h1] = (y[0].astype(F32) + y[1].astype(F32)).astype(BF16)

        @pl.when(has_up)
        def _():
            hid[c][0].start()

        @pl.when(has_dn)
        def _():
            hid[c][1].start()

    def second_conv(c, unit0, unit1):
        if c < chunks:
            @pl.when(has_dn)
            def _():
                hid[c][0].wait_recv()

            @pl.when(has_up)
            def _():
                hid[c][1].wait_recv()

        h0, h1 = sb[c], sb[c + 1]
        size = rows * (h1 - h0)

        def job(accs, kind, q, p):
            weight = ((lambda: w2[1, p, q]), (lambda: w2[2, p, q]), (lambda: w01[p, q]))[kind]
            return weight, [(accs, lambda: hs[min(kind, 1), p : p + rows, h0:h1].reshape(size, chans))]

        jobs = []
        for accs, q, extra in ((unit0, 0, ((0, 0), (0, 1), (0, 2), (1, 0))), (unit1, 2, ((2, 0), (2, 1), (2, 2), (1, 1), (1, 2)))):
            first = [job(accs[kind], kind, q, p) for kind in range(3) for p in range(3)]
            jobs.append(first + [job(accs[4 if kind == 1 else 3], kind, 1, p) for kind, p in extra])
        matmuls(jobs)
        pops = [[pltpu.matmul_pop(a).reshape(rows, h1 - h0, chans) for a in unit] for unit in (unit0, unit1)]
        (one0, two0, mix0, one1, part0), (one2, two2, mix2, mix1, part1) = pops
        inside = slice(PAD + h0, PAD + h1)
        for q, one, two, mix in ((0, one0, two0, mix0), (1, one1, part0 + part1, mix1), (2, one2, two2, mix2)):
            oq[q, :, inside, :] = one + two
            nq[q, :, inside, :] = mix - one
        p0, p1 = pb[c], pb[c + 1]
        ns[:, p0:p1] = shifted_sum(nq, p0, p1).astype(BF16)

        @pl.when(has_next)
        def _():
            part[c].start()

        own = xo[0, 1 : rows + 1, p0:p1].astype(F32) + xo[1, 1 : rows + 1, p0:p1].astype(F32)
        ob[:, p0:p1] = 0.5 * (shifted_sum(oq, p0, p1) + own) + bias2

    def first(c):
        accumulators(functools.partial(first_conv, c), rows * (xb[c + 1] - xb[c]), 4)

    def second(c):
        accumulators(functools.partial(second_conv, c), rows * (sb[c + 1] - sb[c]), 5)

    for stage, c in ORDER:
        (forward, first, second)[stage](c)

    for c in range(pieces):
        @pl.when(has_prev)
        def _():
            part[c].wait_recv()

        p0, p1 = pb[c], pb[c + 1]
        out[0, :, p0:p1] = (ob[:, p0:p1] + 0.5 * nr[:, p0:p1].astype(F32)).astype(BF16)

    @pl.when(has_next)
    def _():
        for c in range(chunks):
            for copy in (*edges[c], middle[c]):
                copy.wait_send()
        for copy in part:
            copy.wait_send()

    @pl.when(has_up)
    def _():
        own_up.wait_send()
        for c in range(chunks):
            hid[c][0].wait_send()

    @pl.when(has_dn)
    def _():
        own_dn.wait_send()
        for c in range(chunks):
            hid[c][1].wait_send()

    @pl.when(has_prev & has_up)
    def _():
        for c in range(chunks):
            fwd[c][0].wait_send()

    @pl.when(has_prev & has_dn)
    def _():
        for c in range(chunks):
            fwd[c][1].wait_send()


def shards(x, w1, b1, w2, b2):
    frames, rows, width, chans = x.shape
    chunks, pieces = (len(bounds(width)[k]) - 1 for k in (0, 3))
    dma = pltpu.SemaphoreType.DMA
    hbm, vmem = pl.BlockSpec(memory_space=pltpu.HBM), pl.BlockSpec(memory_space=pltpu.VMEM)
    extended = pltpu.VMEM((frames, rows + 2, width, chans), BF16)
    taps = pltpu.VMEM((3, rows, width + 2 * PAD, chans), F32)
    flat = pltpu.VMEM((rows, width, chans), BF16)
    return pl.pallas_call(
        kernel,
        out_shape=pltpu.VMEM((1, rows, width, chans), BF16),
        in_specs=[hbm] * 5,
        out_specs=vmem,
        scratch_shapes=[
            extended, extended,
            pltpu.VMEM(w1.shape, BF16), pltpu.VMEM(w2.shape, BF16), pltpu.VMEM(w2.shape[1:], BF16),
            pltpu.VMEM((1, chans), F32), pltpu.VMEM((1, chans), F32),
            pltpu.VMEM((3, frames, rows, width + 2 * PAD, chans), F32),
            extended, taps, taps, pltpu.VMEM((rows, width, chans), F32),
            flat, flat,
            dma((8,)), pltpu.SemaphoreType.REGULAR((2,)),
            dma((3 * chunks,)), dma((3 * chunks,)),
            dma((2,)), dma((2,)),
            dma((2 * chunks,)), dma((2 * chunks,)),
            dma((2 * chunks,)), dma((2 * chunks,)),
            dma((pieces,)), dma((pieces,)),
        ],
        compiler_params=pltpu.CompilerParams(
            collective_id=0, has_side_effects=True, vmem_limit_bytes=67043328 - 600000
        ),
    )(x, w1, b1.reshape(1, chans), w2, b2.reshape(1, chans))


def solution(mesh):
    spec = P(("clips", "tm"), "tile", None, None)
    return jax.shard_map(shards, mesh=mesh, in_specs=(spec, P(), P(), P(), P()), out_specs=spec, check_vma=False)
```
